128 devices in a mesh: depth: 8 (over x, z_hi), screen: 16 (over z_lo, y, core).
Axes of the slice: x: 4, y: 4, z: 4 (z_hi: 2, z_lo: 2; z = z_hi * 2 + z_lo), core: 2. Of those that a mesh axis runs over, the one named last changes fastest.
Arguments:
- voxel_bins: int32 [64, 256, 4096], P('depth', None, 'screen'), may hold values from 0 to 255
- colors: bfloat16 [3, 256], replicated, may hold values from 0 to 2
- opacity: bfloat16 [256], replicated, may hold values from 0 to 1
- slab_order: int32 [16, 8], replicated, may hold values from 0 to 7, each once within a row
Outputs:
- image: float32 [4, 256, 4096], P(None, ('depth', 'screen'))
The draws below stay inside these ranges and needn't reach their ends.
Inputs may be any that keep to these rules, and one draw needn't show every extreme that they name: `slab_order`: every row is a permutation of 0 to 7.
All inputs are finite; a program needn't handle non-finite values.
Results may differ from the reference program's by a relative error of at most 0.0003.
Values sent between devices are 32-bit elements; how exact they have to be, the bound alone decides.
A program may use at most 64 MiB of HBM per device.

```python
import jax
import jax.numpy as jnp
from jax import lax

NBINS = 256
IMG_H = 256
SAMPLES = 64
IMG_W = 4096
DEPTHS = 8
TILES = 16


def place_ends(result, own_key, least, largest):
    extent = result.shape
    index_at = [jax.random.randint(jax.random.fold_in(own_key, axis), (), 0, extent[axis]) for axis in range(len(extent))]
    result = result.at[tuple(index_at)].set(least)
    longest = extent.index(max(extent))
    index_at[longest] = (index_at[longest] + 1) % extent[longest]
    return result.at[tuple(index_at)].set(largest)


def setup_inputs(seed: int = 0) -> dict:
    arg_keys = jax.random.split(jax.random.key(seed), 5)
    voxel_bins = place_ends(jax.random.randint(arg_keys[0], (SAMPLES, IMG_H, IMG_W), 0, NBINS), jax.random.fold_in(arg_keys[0], 1), 0, NBINS - 1).astype(jnp.int32)
    colors = jnp.clip(jax.random.uniform(arg_keys[1], (3, NBINS), jnp.float32, 0.0, 2.0), 0.0, 2.0).astype(jnp.bfloat16)
    opacity = jnp.clip(jax.random.uniform(arg_keys[2], (NBINS,), jnp.float32, 0.0, 1.0), 0.0, 1.0).astype(jnp.bfloat16)
    slab_order = jax.vmap(lambda own: jax.random.permutation(own, DEPTHS))(jax.random.split(arg_keys[3], TILES)).reshape((TILES, DEPTHS)).astype(jnp.int32)
    return dict(voxel_bins=voxel_bins, colors=colors, opacity=opacity, slab_order=slab_order)


def reference(voxel_bins, colors, opacity, slab_order):
    table = jnp.concatenate([colors, opacity[None]], axis=0).astype(jnp.float32)
    sample_total = voxel_bins.shape[0]
    slab_count = slab_order.shape[1]
    tile_count = slab_order.shape[0]
    row_count = voxel_bins.shape[1]
    col_count = voxel_bins.shape[2]
    extinct_rate = 3.0 / sample_total
    slabs = voxel_bins.reshape(slab_count, sample_total // slab_count, row_count, col_count)

    def march(slab):
        def advance(carried, layer):
            passed, color_sum = carried
            values = jnp.take(table, layer, axis=1)
            density = values[3]
            weight = (1.0 - jnp.exp(-extinct_rate * density)) * jnp.exp(-extinct_rate * passed)
            return (passed + density, color_sum + weight[None] * values[:3]), None

        start = (jnp.zeros((row_count, col_count), jnp.float32), jnp.zeros((3, row_count, col_count), jnp.float32))
        (passed, color_sum), ignored = lax.scan(advance, start, slab)
        final_alpha = 1.0 - jnp.exp(-extinct_rate * passed)
        return jnp.concatenate([color_sum, final_alpha[None]], axis=0)

    partials = lax.map(march, slabs)
    pieces = partials.reshape(slab_count, 4, row_count, tile_count, col_count // tile_count)
    acc_color = jnp.zeros((3, row_count, tile_count, col_count // tile_count), jnp.float32)
    acc_alpha = jnp.zeros((row_count, tile_count, col_count // tile_count), jnp.float32)
    for place in range(slab_count):
        select = (slab_order == place).astype(jnp.float32)
        picked = jnp.einsum("ti,icrtw->crtw", select, pieces, precision=lax.Precision.HIGHEST)
        acc_color = acc_color + (1.0 - acc_alpha)[None] * picked[:3]
        acc_alpha = acc_alpha + (1.0 - acc_alpha) * picked[3]
    merged = jnp.concatenate([acc_color, acc_alpha[None]], axis=0)
    return merged.reshape(4, row_count, col_count)
```

```python
import jax
import jax.numpy as jnp
from jax import lax
from jax.experimental import pallas as pl
from jax.experimental.pallas import tpu as pltpu
from jax.sharding import PartitionSpec as P

extinction = 3.0
MESH = pl.DeviceIdType.MESH


def ring(step):
    return min(step, 4 - step)


OFFSETS = sorted(
    [(dx, dz) for dx in range(4) for dz in range(4) if (dx, dz) != (0, 0)],
    key=lambda o: (-(ring(o[0]) + ring(o[1])), (o[0] * 5 + o[1] * 3) % 11),
)
PEERS = len(OFFSETS)
NEAR = [(2, 0), (2, 1), (3, 0), (3, 1), (1, 0), (1, 1), (0, 1)]
SLOTS = len(NEAR)


def coords():
    depth = lax.axis_index("depth")
    screen = lax.axis_index("screen")
    return depth // 2, (depth % 2) * 2 + screen // 8, (screen // 2) % 4, screen % 2


def device(x, z, y, core):
    return {"depth": x * 2 + z // 2, "screen": (z % 2) * 8 + y * 2 + core}


def gather_lanes(table, lanes):
    return jnp.take_along_axis(table, lanes, axis=1, mode="promise_in_bounds")


def shade(bins, tables):
    sums = None
    for layer in bins:
        lanes = layer & 127
        low = layer < 128
        values = [
            jnp.where(low, gather_lanes(tables[2 * ch], lanes), gather_lanes(tables[2 * ch + 1], lanes))
            for ch in range(4)
        ]
        if sums is None:
            sums = values
        else:
            clear = 1.0 - sums[3]
            sums = [s + clear * v for s, v in zip(sums, values)]
    return sums


def regroup(planes, pair):
    low_half = pair < 2
    even = (pair % 2) == 0
    u0 = jnp.where(low_half, planes[0], pltpu.roll(planes[2], 4, 0))
    u1 = jnp.where(low_half, planes[1], pltpu.roll(planes[3], 4, 0))
    v0 = jnp.where(low_half, pltpu.roll(planes[0], 4, 0), planes[2])
    v1 = jnp.where(low_half, pltpu.roll(planes[1], 4, 0), planes[3])
    return [
        jnp.where(even, u0, pltpu.roll(u1, 2, 0)),
        jnp.where(even, pltpu.roll(u0, 6, 0), u1),
        jnp.where(even, v0, pltpu.roll(v1, 2, 0)),
        jnp.where(even, pltpu.roll(v0, 6, 0), v1),
    ]


def kernel(
    vox, table_ref, order_ref, out_ref,
    vin, send_far, send_near, recv_far, recv_sib, recv_other, recv_own, result, landed, place,
    load_sem, self_sem, send_sem, recv_sem, send2_sem, recv2_sem,
):
    x, z, y, core = coords()
    half = y // 2
    me_block = x * 4 + z
    slab = x * 2 + z // 2
    side = z % 2
    sibling = y + 1 - 2 * (y % 2)
    ys = [y, sibling, (y + 2) % 4, (sibling + 2) % 4]
    cores = [core, 1 - core]

    def load(part):
        source = half if part else 1 - half
        return pltpu.make_async_copy(vox.at[:, :, source], vin.at[part], load_sem.at[part])

    load(0).start()
    load(1).start()

    barrier = pltpu.get_barrier_semaphore()
    for dx, dz in OFFSETS:
        pl.semaphore_signal(
            barrier, inc=1, device_id=device((x + dx) % 4, (z + dz) % 4, y, core), device_id_type=MESH
        )
    for yrel, crel in NEAR:
        pl.semaphore_signal(barrier, inc=1, device_id=device(x, z, ys[yrel], cores[crel]), device_id_type=MESH)

    for t in range(2):
        row = t * 8 + y * 2 + core
        places = [order_ref[i, row] for i in range(8)]
        for k in range(8):
            found = jnp.int32(0)
            for i in range(8):
                found = jnp.where(places[i] == k, jnp.int32(i), found)
            place[t * 8 + k] = found

    tables = [jnp.broadcast_to(table_ref[i : i + 1, :], (8, 128)) for i in range(8)]
    pair = lax.broadcasted_iota(jnp.int32, (8, 128), 0) // 2

    def render(part):
        def rows(step, carry):
            for sub in range(2):
                block = step * 2 + sub
                for col in range(2):
                    span = pl.ds(col * 128, 128)
                    bins = [vin[part, j, block, :, span] for j in range(8)]
                    blocks = regroup(shade(bins, tables), pair)
                    for q in range(4):
                        if part == 0:
                            send_far[block, q // 2, q % 2, :, span] = blocks[q]
                        else:
                            send_near[(q // 2 + y) % 2, block, q % 2, :, span] = blocks[q]
            return carry

        lax.fori_loop(0, 8, rows, 0)

    buffers = [
        (lambda b: send_far.at[b], recv_far),
        (lambda b: send_near.at[1, b], recv_sib),
        (lambda b: send_near.at[0, b, 1 - core], recv_other),
        (lambda b: send_near.at[0, b, core], recv_own),
    ]

    def message(group, k):
        dx, dz = OFFSETS[k]
        to_x, to_z = (x + dx) % 4, (z + dz) % 4
        source, target = buffers[group]
        return pltpu.make_async_remote_copy(
            src_ref=source(to_x * 4 + to_z),
            dst_ref=target.at[side, slab],
            send_sem=send_sem.at[group, k],
            recv_sem=recv_sem.at[group, k],
            device_id=device(to_x, to_z, y, core),
            device_id_type=MESH,
        )

    def keep(group):
        source, target = buffers[group]
        return pltpu.make_async_copy(source(me_block), target.at[side, slab], self_sem.at[group])

    def send(group):
        for k in range(PEERS):
            message(group, k).start()
        keep(group).start()

    def arrive(group):
        for k in range(PEERS):
            message(group, k).wait_recv()
        keep(group).wait()

    load(0).wait()
    render(0)
    pl.semaphore_wait(barrier, PEERS + SLOTS)
    send(0)
    load(1).wait()
    render(1)
    send(1)
    send(2)
    send(3)

    alpha_rows = 6 + lax.broadcasted_iota(jnp.int32, (8, 128), 0) % 2

    def over(read, store):
        for t in range(2):
            for col in range(2):
                span = pl.ds(col * 128, 128)
                total = read(t, place[t * 8], span)
                for k in range(1, 8):
                    alpha = jnp.take_along_axis(total, alpha_rows, axis=0, mode="promise_in_bounds")
                    total = total + (1.0 - alpha) * read(t, place[t * 8 + k], span)
                store(t, span, total)

    def forward(slot):
        yrel, crel = NEAR[slot]
        return pltpu.make_async_remote_copy(
            src_ref=result.at[slot],
            dst_ref=landed.at[slot],
            send_sem=send2_sem.at[slot],
            recv_sem=recv2_sem.at[slot],
            device_id=device(x, z, ys[yrel], cores[crel]),
            device_id_type=MESH,
        )

    def pass_on(slot, read):
        def store(t, span, total):
            result[slot, t, :, span] = total

        over(read, store)
        forward(slot).start()

    arrive(0)
    for slot in range(4):
        yrel, crel = NEAR[slot]
        pass_on(slot, lambda t, s, span: recv_far[t, s, ys[yrel] % 2, cores[crel], :, span])
    arrive(1)
    for slot in range(4, 6):
        crel = NEAR[slot][1]
        pass_on(slot, lambda t, s, span: recv_sib[t, s, cores[crel], :, span])
    arrive(2)
    pass_on(6, lambda t, s, span: recv_other[t, s, :, span])

    def put(slot):
        yrel, crel = NEAR[slot]
        forward(slot).wait_recv()
        for t in range(2):
            out_ref[t * 8 + ys[yrel] * 2 + cores[crel]] = landed[slot, t]

    for slot in range(4):
        put(slot)
    arrive(3)

    def store_own(t, span, total):
        out_ref[t * 8 + y * 2 + core, :, span] = total

    over(lambda t, s, span: recv_own[t, s, :, span], store_own)
    for slot in range(4, SLOTS):
        put(slot)

    for group in range(4):
        for k in range(PEERS):
            message(group, k).wait_send()
    for slot in range(SLOTS):
        forward(slot).wait_send()


def local(voxel_bins, colors, opacity, slab_order):
    rate = extinction / (voxel_bins.shape[0] * lax.axis_size("depth"))
    alpha = -jnp.expm1(-rate * opacity.astype(jnp.float32))
    shaded = jnp.concatenate([colors.astype(jnp.float32) * alpha[None], alpha[None]], axis=0)
    table = shaded.reshape(8, 128)
    vox = voxel_bins.reshape(8, 16, 2, 8, 256)
    f32 = jnp.float32
    out = pl.pallas_call(
        kernel,
        out_shape=jax.ShapeDtypeStruct((16, 8, 256), f32),
        in_specs=[
            pl.BlockSpec(memory_space=pl.ANY),
            pl.BlockSpec(memory_space=pltpu.VMEM),
            pl.BlockSpec(memory_space=pltpu.SMEM),
        ],
        out_specs=pl.BlockSpec(memory_space=pltpu.VMEM),
        scratch_shapes=[
            pltpu.VMEM((2, 8, 16, 8, 256), jnp.int32),
            pltpu.VMEM((16, 2, 2, 8, 256), f32),
            pltpu.VMEM((2, 16, 2, 8, 256), f32),
            pltpu.VMEM((2, 8, 2, 2, 8, 256), f32),
            pltpu.VMEM((2, 8, 2, 8, 256), f32),
            pltpu.VMEM((2, 8, 8, 256), f32),
            pltpu.VMEM((2, 8, 8, 256), f32),
            pltpu.VMEM((SLOTS, 2, 8, 256), f32),
            pltpu.VMEM((SLOTS, 2, 8, 256), f32),
            pltpu.SMEM((16,), jnp.int32),
            pltpu.SemaphoreType.DMA((2,)),
            pltpu.SemaphoreType.DMA((4,)),
            pltpu.SemaphoreType.DMA((4, PEERS)),
            pltpu.SemaphoreType.DMA((4, PEERS)),
            pltpu.SemaphoreType.DMA((SLOTS,)),
            pltpu.SemaphoreType.DMA((SLOTS,)),
        ],
        compiler_params=pltpu.CompilerParams(collective_id=0, has_side_effects=True),
        name="render_exchange",
    )(vox, table, slab_order.T)
    out = out.reshape(16, 4, 2, 256)
    return jnp.transpose(out, (1, 2, 0, 3)).reshape(4, 2, 4096)


def solution(mesh):
    placed = (P("depth", None, "screen"), P(), P(), P())
    return jax.shard_map(
        local,
        mesh=mesh,
        in_specs=placed,
        out_specs=P(None, ("depth", "screen"), None),
        check_vma=False,
    )
```

```python
import jax
import jax.numpy as jnp
from jax import lax
from jax.experimental import pallas as pl
from jax.experimental.pallas import tpu as pltpu
from jax.sharding import PartitionSpec as P

extinction = 3.0
MESH = pl.DeviceIdType.MESH


def ring(step):
    return min(step, 4 - step)


OFFSETS = sorted(
    [(dx, dz) for dx in range(4) for dz in range(4)],
    key=lambda o: (-(ring(o[0]) + ring(o[1])), (o[0] * 5 + o[1] * 3) % 11),
)
PEERS = len(OFFSETS) - 1
NEAR = [(2, 0), (2, 1), (3, 0), (3, 1), (1, 0), (1, 1), (0, 1), (0, 0)]
SLOTS = len(NEAR) - 1


def coords():
    depth = lax.axis_index("depth")
    screen = lax.axis_index("screen")
    return depth // 2, (depth % 2) * 2 + screen // 8, (screen // 2) % 4, screen % 2


def device(x, z, y, core):
    return {"depth": x * 2 + z // 2, "screen": (z % 2) * 8 + y * 2 + core}


def gather_lanes(table, lanes):
    numbers = lax.GatherDimensionNumbers(
        offset_dims=(),
        collapsed_slice_dims=(1,),
        start_index_map=(1,),
        operand_batching_dims=(0,),
        start_indices_batching_dims=(0,),
    )
    return lax.gather(
        table, lanes[..., None], numbers, slice_sizes=(1, 1), mode=lax.GatherScatterMode.PROMISE_IN_BOUNDS
    )


def shade(patches, tables):
    sums = [None] * len(patches)
    for j in range(len(patches[0])):
        for i, bins in enumerate(patches):
            lanes = bins[j] & 127
            low = bins[j] < 128
            values = [
                jnp.where(low, gather_lanes(tables[2 * ch], lanes), gather_lanes(tables[2 * ch + 1], lanes))
                for ch in range(4)
            ]
            if j == 0:
                sums[i] = values
            else:
                clear = 1.0 - sums[i][3]
                sums[i] = [s + clear * v for s, v in zip(sums[i], values)]
    return sums


def regroup(planes, pair):
    low_half = pair < 2
    even = (pair % 2) == 0
    u0 = jnp.where(low_half, planes[0], pltpu.roll(planes[2], 4, 0))
    u1 = jnp.where(low_half, planes[1], pltpu.roll(planes[3], 4, 0))
    v0 = jnp.where(low_half, pltpu.roll(planes[0], 4, 0), planes[2])
    v1 = jnp.where(low_half, pltpu.roll(planes[1], 4, 0), planes[3])
    return [
        jnp.where(even, u0, pltpu.roll(u1, 2, 0)),
        jnp.where(even, pltpu.roll(u0, 6, 0), u1),
        jnp.where(even, v0, pltpu.roll(v1, 2, 0)),
        jnp.where(even, pltpu.roll(v0, 6, 0), v1),
    ]


def kernel(
    vox, colors, opacity, order, out_ref,
    vin, colors_in, opacity_in, order_in, send_far, send_near, recv_far, recv_sib, recv_other, recv_own, result, landed,
    place, small_sem, load_sem, self_sem, send_sem, recv_sem, send2_sem, recv2_sem,
):
    x, z, y, core = coords()
    half = y // 2
    slab = x * 2 + z // 2
    side = z % 2
    sibling = y + 1 - 2 * (y % 2)
    ys = [y, sibling, (y + 2) % 4, (sibling + 2) % 4]
    cores = [core, 1 - core]

    def load(part):
        source = half if part else 1 - half
        return pltpu.make_async_copy(vox.at[:, :, source], vin.at[part], load_sem.at[part])

    small = [
        pltpu.make_async_copy(colors, colors_in, small_sem.at[0]),
        pltpu.make_async_copy(opacity, opacity_in, small_sem.at[1]),
        pltpu.make_async_copy(order, order_in, small_sem.at[2]),
    ]
    for copy in small[:2]:
        copy.start()
    load(0).start()
    load(1).start()
    small[2].start()

    barrier = pltpu.get_barrier_semaphore()
    for dx, dz in OFFSETS[:-1]:
        pl.semaphore_signal(
            barrier, inc=1, device_id=device((x + dx) % 4, (z + dz) % 4, y, core), device_id_type=MESH
        )
    for yrel, crel in NEAR[:-1]:
        pl.semaphore_signal(barrier, inc=1, device_id=device(x, z, ys[yrel], cores[crel]), device_id_type=MESH)

    small[0].wait()
    small[1].wait()
    alpha = 1.0 - jnp.exp(-(extinction / 64) * opacity_in[...].astype(jnp.float32).reshape(1, 256))
    shaded = colors_in[...].astype(jnp.float32) * alpha
    tables = [
        jnp.broadcast_to((shaded[ch : ch + 1] if ch < 3 else alpha)[:, part * 128 : part * 128 + 128], (8, 128))
        for ch in range(4)
        for part in range(2)
    ]
    pair = lax.broadcasted_iota(jnp.int32, (8, 128), 0) // 2

    def place_of(k):
        dx, dz = OFFSETS[k]
        return (x + dx) % 4, (z + dz) % 4

    def render(part, ks):
        blocks = [to_x * 4 + to_z for to_x, to_z in map(place_of, ks)]
        spots = [(b, pl.ds(col * 128, 128)) for b in blocks for col in range(2)]
        for (b, span), planes in zip(
            spots, shade([[vin[part, j, b, :, span] for j in range(8)] for b, span in spots], tables)
        ):
            for q, rows in enumerate(regroup(planes, pair)):
                if part == 0:
                    send_far[b, q // 2, q % 2, :, span] = rows
                else:
                    send_near[(q // 2 + y) % 2, b, q % 2, :, span] = rows

    buffers = [
        (lambda b: send_far.at[b], recv_far),
        (lambda b: send_near.at[1, b], recv_sib),
        (lambda b: send_near.at[0, b, 1 - core], recv_other),
        (lambda b: send_near.at[0, b, core], recv_own),
    ]

    def message(group, k):
        to_x, to_z = place_of(k)
        source, target = buffers[group]
        return pltpu.make_async_remote_copy(
            src_ref=source(to_x * 4 + to_z),
            dst_ref=target.at[side, slab],
            send_sem=send_sem.at[group, k],
            recv_sem=recv_sem.at[group, k],
            device_id=device(to_x, to_z, y, core),
            device_id_type=MESH,
        )

    def keep(group):
        source, target = buffers[group]
        return pltpu.make_async_copy(source(x * 4 + z), target.at[side, slab], self_sem.at[group])

    def send(group, k):
        if k < PEERS:
            message(group, k).start()
        else:
            keep(group).start()

    def arrive(group):
        for k in range(PEERS):
            message(group, k).wait_recv()
        keep(group).wait()

    load(0).wait()
    for k in range(0, PEERS + 1, 2):
        render(0, [k, k + 1])
        if k == 0:
            pl.semaphore_wait(barrier, PEERS + SLOTS)
        send(0, k)
        send(0, k + 1)
    load(1).wait()
    for k in range(0, PEERS + 1, 2):
        render(1, [k, k + 1])
        send(1, k)
        send(1, k + 1)
    for group in (2, 3):
        for k in range(PEERS + 1):
            send(group, k)

    small[2].wait()
    for t in range(2):
        row = t * 8 + y * 2 + core
        places = [order_in[i, row] for i in range(8)]
        for k in range(8):
            found = jnp.int32(0)
            for i in range(8):
                found = jnp.where(places[i] == k, jnp.int32(i), found)
            place[t * 8 + k] = found

    alpha_rows = 6 + lax.broadcasted_iota(jnp.int32, (8, 128), 0) % 2

    def over(read, store):
        for t in range(2):
            for col in range(2):
                span = pl.ds(col * 128, 128)
                total = read(t, place[t * 8], span)
                for k in range(1, 8):
                    alpha = jnp.take_along_axis(total, alpha_rows, axis=0, mode="promise_in_bounds")
                    total = total + (1.0 - alpha) * read(t, place[t * 8 + k], span)
                store(t, span, total)

    def forward(slot):
        yrel, crel = NEAR[slot]
        return pltpu.make_async_remote_copy(
            src_ref=result.at[yrel, cores[crel]],
            dst_ref=landed.at[yrel, core],
            send_sem=send2_sem.at[slot],
            recv_sem=recv2_sem.at[slot],
            device_id=device(x, z, ys[yrel], cores[crel]),
            device_id_type=MESH,
        )

    def pass_on(slot, read):
        yrel, crel = NEAR[slot]

        def store(t, span, total):
            result[yrel, cores[crel], t, :, span] = total

        over(read, store)
        if slot < SLOTS:
            forward(slot).start()

    def put(yrel):
        for t in range(2):
            blocks = [landed[yrel, c, t, :, pl.ds(col * 128, 128)] for c in range(2) for col in range(2)]
            for ch, rows in enumerate(regroup(blocks, pair)):
                out_ref[ch * 8 + t * 4 + ys[yrel]] = rows

    arrive(0)
    for slot in range(4):
        yrel, crel = NEAR[slot]
        pass_on(slot, lambda t, s, span: recv_far[t, s, ys[yrel] % 2, cores[crel], :, span])
    arrive(1)
    for slot in range(4, 6):
        crel = NEAR[slot][1]
        pass_on(slot, lambda t, s, span: recv_sib[t, s, cores[crel], :, span])
    arrive(2)
    pass_on(6, lambda t, s, span: recv_other[t, s, :, span])
    for slot in range(4):
        forward(slot).wait_recv()
    put(2)
    put(3)
    arrive(3)

    def store_own(t, span, total):
        landed[0, core, t, :, span] = total

    over(lambda t, s, span: recv_own[t, s, :, span], store_own)
    for slot in range(4, SLOTS):
        forward(slot).wait_recv()
    put(1)
    put(0)

    for group in range(4):
        for k in range(PEERS):
            message(group, k).wait_send()
    for slot in range(SLOTS):
        forward(slot).wait_send()


def local(voxel_bins, colors, opacity, slab_order):
    f32 = jnp.float32
    out = pl.pallas_call(
        kernel,
        out_shape=jax.ShapeDtypeStruct((32, 8, 128), f32),
        in_specs=[pl.BlockSpec(memory_space=pl.ANY)] * 4,
        out_specs=pl.BlockSpec(memory_space=pltpu.VMEM),
        scratch_shapes=[
            pltpu.VMEM((2, 8, 16, 8, 256), jnp.int32),
            pltpu.VMEM((3, 256), jnp.bfloat16),
            pltpu.VMEM((256,), jnp.bfloat16),
            pltpu.SMEM((8, 16), jnp.int32),
            pltpu.VMEM((16, 2, 2, 8, 256), f32),
            pltpu.VMEM((2, 16, 2, 8, 256), f32),
            pltpu.VMEM((2, 8, 2, 2, 8, 256), f32),
            pltpu.VMEM((2, 8, 2, 8, 256), f32),
            pltpu.VMEM((2, 8, 8, 256), f32),
            pltpu.VMEM((2, 8, 8, 256), f32),
            pltpu.VMEM((4, 2, 2, 8, 256), f32),
            pltpu.VMEM((4, 2, 2, 8, 256), f32),
            pltpu.SMEM((16,), jnp.int32),
            pltpu.SemaphoreType.DMA((3,)),
            pltpu.SemaphoreType.DMA((2,)),
            pltpu.SemaphoreType.DMA((4,)),
            pltpu.SemaphoreType.DMA((4, PEERS)),
            pltpu.SemaphoreType.DMA((4, PEERS)),
            pltpu.SemaphoreType.DMA((SLOTS,)),
            pltpu.SemaphoreType.DMA((SLOTS,)),
        ],
        compiler_params=pltpu.CompilerParams(collective_id=0, has_side_effects=True),
        name="render_exchange",
    )(voxel_bins.reshape(8, 16, 2, 8, 256), colors, opacity, slab_order.T)
    return jnp.transpose(out.reshape(4, 32, 2, 128), (0, 2, 1, 3)).reshape(4, 2, 4096)


def solution(mesh):
    placed = (P("depth", None, "screen"), P(), P(), P())
    return jax.shard_map(
        local,
        mesh=mesh,
        in_specs=placed,
        out_specs=P(None, ("depth", "screen"), None),
        check_vma=False,
    )
```

```python
import jax
import jax.numpy as jnp
from jax import lax
from jax.experimental import pallas as pl
from jax.experimental.pallas import tpu as pltpu
from jax.sharding import PartitionSpec as P

extinction = 3.0
MESH = pl.DeviceIdType.MESH


def ring(step):
    return min(step, 4 - step)


OFFSETS = sorted(
    [(dx, dz) for dx in range(4) for dz in range(4)],
    key=lambda o: (o == (0, 0), (o[0] * 5 + o[1] * 3) % 11),
)
PEERS = len(OFFSETS) - 1
NEAR = [(2, 0), (2, 1), (3, 0), (3, 1), (1, 0), (1, 1), (0, 1), (0, 0)]
SLOTS = len(NEAR) - 1


def coords():
    depth = lax.axis_index("depth")
    screen = lax.axis_index("screen")
    return depth // 2, (depth % 2) * 2 + screen // 8, (screen // 2) % 4, screen % 2


def device(x, z, y, core):
    return {"depth": x * 2 + z // 2, "screen": (z % 2) * 8 + y * 2 + core}


def gather_lanes(table, lanes):
    numbers = lax.GatherDimensionNumbers(
        offset_dims=(),
        collapsed_slice_dims=(1,),
        start_index_map=(1,),
        operand_batching_dims=(0,),
        start_indices_batching_dims=(0,),
    )
    return lax.gather(
        table, lanes[..., None], numbers, slice_sizes=(1, 1), mode=lax.GatherScatterMode.PROMISE_IN_BOUNDS
    )


def shade(patches, tables):
    sums = [None] * len(patches)
    for j in range(len(patches[0])):
        for i, bins in enumerate(patches):
            lanes = bins[j] & 127
            low = bins[j] < 128
            values = [
                jnp.where(low, gather_lanes(tables[2 * ch], lanes), gather_lanes(tables[2 * ch + 1], lanes))
                for ch in range(4)
            ]
            if j == 0:
                sums[i] = values
            else:
                clear = 1.0 - sums[i][3]
                sums[i] = [s + clear * v for s, v in zip(sums[i], values)]
    return sums


def regroup(planes, pair):
    low_half = pair < 2
    even = (pair % 2) == 0
    u0 = jnp.where(low_half, planes[0], pltpu.roll(planes[2], 4, 0))
    u1 = jnp.where(low_half, planes[1], pltpu.roll(planes[3], 4, 0))
    v0 = jnp.where(low_half, pltpu.roll(planes[0], 4, 0), planes[2])
    v1 = jnp.where(low_half, pltpu.roll(planes[1], 4, 0), planes[3])
    return [
        jnp.where(even, u0, pltpu.roll(u1, 2, 0)),
        jnp.where(even, pltpu.roll(u0, 6, 0), u1),
        jnp.where(even, v0, pltpu.roll(v1, 2, 0)),
        jnp.where(even, pltpu.roll(v0, 6, 0), v1),
    ]


def kernel(
    vox, colors, opacity, order, out_ref,
    vin, colors_in, opacity_in, order_in, send_far, send_near, recv_far, recv_sib, recv_other, recv_own, result, landed,
    place, small_sem, load_sem, send_sem, recv_sem, send2_sem, recv2_sem,
):
    x, z, y, core = coords()
    half = y // 2
    slab = x * 2 + z // 2
    side = z % 2
    sibling = y + 1 - 2 * (y % 2)
    ys = [y, sibling, (y + 2) % 4, (sibling + 2) % 4]
    cores = [core, 1 - core]

    def load(part):
        source = half if part else 1 - half
        return pltpu.make_async_copy(vox.at[:, :, source], vin.at[part], load_sem.at[part])

    small = [
        pltpu.make_async_copy(colors, colors_in, small_sem.at[0]),
        pltpu.make_async_copy(opacity, opacity_in, small_sem.at[1]),
        pltpu.make_async_copy(order, order_in, small_sem.at[2]),
    ]
    for copy in small[:2]:
        copy.start()
    load(0).start()
    load(1).start()
    small[2].start()

    barrier = pltpu.get_barrier_semaphore()
    for dx, dz in OFFSETS[:-1]:
        pl.semaphore_signal(
            barrier, inc=1, device_id=device((x + dx) % 4, (z + dz) % 4, y, core), device_id_type=MESH
        )
    for yrel, crel in NEAR[:-1]:
        pl.semaphore_signal(barrier, inc=1, device_id=device(x, z, ys[yrel], cores[crel]), device_id_type=MESH)

    small[0].wait()
    small[1].wait()
    alpha = 1.0 - jnp.exp(-(extinction / 64) * opacity_in[...].astype(jnp.float32).reshape(1, 256))
    shaded = colors_in[...].astype(jnp.float32) * alpha
    tables = [
        jnp.broadcast_to((shaded[ch : ch + 1] if ch < 3 else alpha)[:, part * 128 : part * 128 + 128], (8, 128))
        for ch in range(4)
        for part in range(2)
    ]
    pair = lax.broadcasted_iota(jnp.int32, (8, 128), 0) // 2

    def place_of(k):
        dx, dz = OFFSETS[k]
        return (x + dx) % 4, (z + dz) % 4

    def render(part, ks):
        blocks = [to_x * 4 + to_z for to_x, to_z in map(place_of, ks)]
        spots = [(b, pl.ds(col * 128, 128)) for b in blocks for col in range(2)]
        for (b, span), planes in zip(
            spots, shade([[vin[part, j, b, :, span] for j in range(8)] for b, span in spots], tables)
        ):
            for q, rows in enumerate(regroup(planes, pair)):
                if part == 0:
                    send_far[b, q // 2, q % 2, :, span] = rows
                else:
                    send_near[(q // 2 + y) % 2, b, q % 2, :, span] = rows

    buffers = [
        (lambda b: send_far.at[b], recv_far),
        (lambda b: send_near.at[1, b], recv_sib),
        (lambda b: send_near.at[0, b, 1 - core], recv_other),
        (lambda b: send_near.at[0, b, core], recv_own),
    ]

    def message(group, k):
        to_x, to_z = place_of(k)
        source, target = buffers[group]
        return pltpu.make_async_remote_copy(
            src_ref=source(to_x * 4 + to_z),
            dst_ref=target.at[side, slab],
            send_sem=send_sem.at[min(group, 2)],
            recv_sem=recv_sem.at[group],
            device_id=device(to_x, to_z, y, core),
            device_id_type=MESH,
        )

    def keep(group):
        source, target = buffers[group]
        return pltpu.make_async_copy(source(x * 4 + z), target.at[side, slab], recv_sem.at[group])

    def send(group, k):
        if k < PEERS:
            message(group, k).start()
        else:
            keep(group).start()

    def arrive(group):
        whole = buffers[group][1]
        pltpu.make_async_copy(whole, whole, recv_sem.at[group]).wait()

    load(0).wait()
    for k in range(0, PEERS + 1, 2):
        render(0, [k, k + 1])
        if k == 0:
            pl.semaphore_wait(barrier, PEERS + SLOTS)
        send(0, k)
        send(0, k + 1)
    load(1).wait()
    for k in range(0, PEERS + 1, 2):
        render(1, [k, k + 1])
        send(1, k)
        send(1, k + 1)
    for group in (2, 3):
        for k in range(PEERS + 1):
            send(group, k)

    small[2].wait()
    for t in range(2):
        row = t * 8 + y * 2 + core
        places = [order_in[i, row] for i in range(8)]
        for k in range(8):
            found = jnp.int32(0)
            for i in range(8):
                found = jnp.where(places[i] == k, jnp.int32(i), found)
            place[t * 8 + k] = found

    alpha_rows = 6 + lax.broadcasted_iota(jnp.int32, (8, 128), 0) % 2

    def over(read, store):
        for t in range(2):
            for col in range(2):
                span = pl.ds(col * 128, 128)
                total = read(t, place[t * 8], span)
                for k in range(1, 8):
                    alpha = jnp.take_along_axis(total, alpha_rows, axis=0, mode="promise_in_bounds")
                    total = total + (1.0 - alpha) * read(t, place[t * 8 + k], span)
                store(t, span, total)

    def forward(slot):
        yrel, crel = NEAR[slot]
        return pltpu.make_async_remote_copy(
            src_ref=result.at[slot],
            dst_ref=landed.at[yrel * 2 + core],
            send_sem=send2_sem.at[0],
            recv_sem=recv2_sem.at[slot // 4 + slot // 6],
            device_id=device(x, z, ys[yrel], cores[crel]),
            device_id_type=MESH,
        )

    def pass_on(slot, read):
        def store(t, span, total):
            result[slot, t, :, span] = total

        over(read, store)
        forward(slot).start()

    def land(group):
        part = landed.at[(pl.ds(4, 4), pl.ds(2, 2), pl.ds(0, 1))[group]]
        pltpu.make_async_copy(part, part, recv2_sem.at[group]).wait()

    def put(yrel):
        for t in range(2):
            blocks = [landed[yrel * 2 + c, t, :, pl.ds(col * 128, 128)] for c in range(2) for col in range(2)]
            for ch, rows in enumerate(regroup(blocks, pair)):
                out_ref[ch * 8 + t * 4 + ys[yrel]] = rows

    arrive(0)
    for slot in range(4):
        yrel, crel = NEAR[slot]
        pass_on(slot, lambda t, s, span: recv_far[t, s, ys[yrel] % 2, cores[crel], :, span])
    arrive(1)
    for slot in range(4, 6):
        crel = NEAR[slot][1]
        pass_on(slot, lambda t, s, span: recv_sib[t, s, cores[crel], :, span])
    arrive(2)
    pass_on(6, lambda t, s, span: recv_other[t, s, :, span])
    land(0)
    put(2)
    put(3)
    arrive(3)

    def store_own(t, span, total):
        landed[core, t, :, span] = total

    over(lambda t, s, span: recv_own[t, s, :, span], store_own)
    land(1)
    put(1)
    land(2)
    put(0)

    sent = [send_far.at[pl.ds(0, PEERS)], send_near.at[1, pl.ds(0, PEERS)], send_near.at[0, pl.ds(0, PEERS)]]
    for group, part in enumerate(sent):
        pltpu.make_async_copy(part, part, send_sem.at[group]).wait()
    part = result.at[pl.ds(0, SLOTS)]
    pltpu.make_async_copy(part, part, send2_sem.at[0]).wait()


def local(voxel_bins, colors, opacity, slab_order):
    f32 = jnp.float32
    out = pl.pallas_call(
        kernel,
        out_shape=pltpu.VMEM((32, 8, 128), f32),
        in_specs=[pl.BlockSpec(memory_space=pl.ANY)] * 4,
        out_specs=pl.BlockSpec(memory_space=pltpu.VMEM),
        scratch_shapes=[
            pltpu.VMEM((2, 8, 16, 8, 256), jnp.int32),
            pltpu.VMEM((3, 256), jnp.bfloat16),
            pltpu.VMEM((256,), jnp.bfloat16),
            pltpu.SMEM((8, 16), jnp.int32),
            pltpu.VMEM((16, 2, 2, 8, 256), f32),
            pltpu.VMEM((2, 16, 2, 8, 256), f32),
            pltpu.VMEM((2, 8, 2, 2, 8, 256), f32),
            pltpu.VMEM((2, 8, 2, 8, 256), f32),
            pltpu.VMEM((2, 8, 8, 256), f32),
            pltpu.VMEM((2, 8, 8, 256), f32),
            pltpu.VMEM((8, 2, 8, 256), f32),
            pltpu.VMEM((8, 2, 8, 256), f32),
            pltpu.SMEM((16,), jnp.int32),
            pltpu.SemaphoreType.DMA((3,)),
            pltpu.SemaphoreType.DMA((2,)),
            pltpu.SemaphoreType.DMA((3,)),
            pltpu.SemaphoreType.DMA((4,)),
            pltpu.SemaphoreType.DMA((1,)),
            pltpu.SemaphoreType.DMA((3,)),
        ],
        compiler_params=pltpu.CompilerParams(collective_id=0, has_side_effects=True),
        name="render_exchange",
    )(voxel_bins.reshape(8, 16, 2, 8, 256), colors, opacity, slab_order.T)
    return jnp.transpose(out.reshape(4, 32, 2, 128), (0, 2, 1, 3)).reshape(4, 2, 4096)


def solution(mesh):
    placed = (P("depth", None, "screen"), P(), P(), P())
    return jax.shard_map(
        local,
        mesh=mesh,
        in_specs=placed,
        out_specs=P(None, ("depth", "screen"), None),
        check_vma=False,
    )
```

```python
import jax
import jax.numpy as jnp
from jax import lax
from jax.experimental import pallas as pl
from jax.experimental.pallas import tpu as pltpu
from jax.sharding import PartitionSpec as P

extinction = 3.0
MESH = pl.DeviceIdType.MESH


def ring(step):
    return min(step, 4 - step)


OFFSETS = sorted(
    [(dx, dz) for dx in range(4) for dz in range(4)],
    key=lambda o: (o == (0, 0), (o[0] * 5 + o[1] * 3) % 11),
)
PEERS = len(OFFSETS) - 1
NEAR = [(2, 0), (2, 1), (3, 0), (3, 1), (1, 0), (1, 1), (0, 1), (0, 0)]
SLOTS = len(NEAR) - 1
GROUPS = [(0, 1, 2, 3), (4, 5), (6,), (7,)]


def coords():
    depth = lax.axis_index("depth")
    screen = lax.axis_index("screen")
    return depth // 2, (depth % 2) * 2 + screen // 8, (screen // 2) % 4, screen % 2


def device(x, z, y, core):
    return {"depth": x * 2 + z // 2, "screen": (z % 2) * 8 + y * 2 + core}


def gather_lanes(table, lanes):
    numbers = lax.GatherDimensionNumbers(
        offset_dims=(),
        collapsed_slice_dims=(1,),
        start_index_map=(1,),
        operand_batching_dims=(0,),
        start_indices_batching_dims=(0,),
    )
    return lax.gather(
        table, lanes[..., None], numbers, slice_sizes=(1, 1), mode=lax.GatherScatterMode.PROMISE_IN_BOUNDS
    )


def shade(patches, tables):
    sums = [None] * len(patches)
    for j in range(len(patches[0])):
        for i, bins in enumerate(patches):
            lanes = bins[j] & 127
            low = bins[j] < 128
            values = [
                jnp.where(low, gather_lanes(tables[2 * ch], lanes), gather_lanes(tables[2 * ch + 1], lanes))
                for ch in range(4)
            ]
            if j == 0:
                sums[i] = values
            else:
                clear = 1.0 - sums[i][3]
                sums[i] = [s + clear * v for s, v in zip(sums[i], values)]
    return sums


def regroup(planes, pair):
    low_half = pair < 2
    even = (pair % 2) == 0
    u0 = jnp.where(low_half, planes[0], pltpu.roll(planes[2], 4, 0))
    u1 = jnp.where(low_half, planes[1], pltpu.roll(planes[3], 4, 0))
    v0 = jnp.where(low_half, pltpu.roll(planes[0], 4, 0), planes[2])
    v1 = jnp.where(low_half, pltpu.roll(planes[1], 4, 0), planes[3])
    return [
        jnp.where(even, u0, pltpu.roll(u1, 2, 0)),
        jnp.where(even, pltpu.roll(u0, 6, 0), u1),
        jnp.where(even, v0, pltpu.roll(v1, 2, 0)),
        jnp.where(even, pltpu.roll(v0, 6, 0), v1),
    ]


def kernel(
    vox, colors, opacity, order, out_ref,
    vin, colors_in, opacity_in, order_in, packed, result, landed, place, small_sem, load_sem, send_sem, recv_sem,
    send2_sem, recv2_sem, *received
):
    x, z, y, core = coords()
    half = y // 2
    slab = x * 2 + z // 2
    side = z % 2
    sibling = y + 1 - 2 * (y % 2)
    ys = [y, sibling, (y + 2) % 4, (sibling + 2) % 4]
    cores = [core, 1 - core]

    barrier = pltpu.get_barrier_semaphore()
    for dx, dz in sorted(OFFSETS[:-1], key=lambda o: -(ring(o[0]) + ring(o[1]))):
        pl.semaphore_signal(
            barrier, inc=1, device_id=device((x + dx) % 4, (z + dz) % 4, y, core), device_id_type=MESH
        )
    for yrel, crel in NEAR[:-1]:
        pl.semaphore_signal(barrier, inc=1, device_id=device(x, z, ys[yrel], cores[crel]), device_id_type=MESH)

    def load(part):
        source = half if part else 1 - half
        return pltpu.make_async_copy(vox.at[:, :, source], vin.at[part], load_sem.at[part])

    small = [
        pltpu.make_async_copy(colors, colors_in, small_sem.at[0]),
        pltpu.make_async_copy(opacity, opacity_in, small_sem.at[1]),
        pltpu.make_async_copy(order, order_in, small_sem.at[2]),
    ]
    for copy in small[:2]:
        copy.start()
    load(0).start()
    load(1).start()
    small[2].start()

    small[0].wait()
    small[1].wait()
    alpha = 1.0 - jnp.exp(-(extinction / 64) * opacity_in[...].astype(jnp.float32).reshape(1, 256))
    shaded = colors_in[...].astype(jnp.float32) * alpha
    tables = [
        jnp.broadcast_to((shaded[ch : ch + 1] if ch < 3 else alpha)[:, part * 128 : part * 128 + 128], (8, 128))
        for ch in range(4)
        for part in range(2)
    ]
    pair = lax.broadcasted_iota(jnp.int32, (8, 128), 0) // 2

    def place_of(k):
        dx, dz = OFFSETS[k]
        return (x + dx) % 4, (z + dz) % 4

    def render(part, ks):
        blocks = [to_x * 4 + to_z for to_x, to_z in map(place_of, ks)]
        spots = [(b, pl.ds(col * 128, 128)) for b in blocks for col in range(2)]
        for (b, span), planes in zip(
            spots, shade([[vin[part, j, b, :, span] for j in range(8)] for b, span in spots], tables)
        ):
            for q, rows in enumerate(regroup(planes, pair)):
                rel, crel = (q // 2 + y) % 2, (q + core) % 2
                slot = rel * (4 + crel) + (1 - rel) * (7 - crel) if part else rel * 2 + crel
                packed[b, slot, :, span] = rows

    def ends(group, b):
        slots = GROUPS[group]
        return packed.at[b, pl.ds(slots[0], len(slots))], received[group].at[side, slab]

    def message(group, k):
        to_x, to_z = place_of(k)
        source, target = ends(group, to_x * 4 + to_z)
        return pltpu.make_async_remote_copy(
            src_ref=source,
            dst_ref=target,
            send_sem=send_sem.at[0],
            recv_sem=recv_sem.at[group],
            device_id=device(to_x, to_z, y, core),
            device_id_type=MESH,
        )

    def keep(group):
        source, target = ends(group, x * 4 + z)
        return pltpu.make_async_copy(source, target, recv_sem.at[group])

    def send(group, k):
        if k < PEERS:
            message(group, k).start()
        else:
            keep(group).start()

    def arrive(group):
        whole = received[group]
        pltpu.make_async_copy(whole, whole, recv_sem.at[group]).wait()

    for part in range(2):
        load(part).wait()
        mine = [g for g, slots in enumerate(GROUPS) if (slots[-1] > 3) == bool(part)]
        for k in range(0, PEERS + 1, 2):
            render(part, [k, k + 1])
            if part == 0 and k == 0:
                pl.semaphore_wait(barrier, PEERS + SLOTS)
            for group in mine[:1]:
                send(group, k)
                send(group, k + 1)
        for group in mine[1:]:
            for k in range(PEERS + 1):
                send(group, k)

    small[2].wait()
    for t in range(2):
        row = t * 8 + y * 2 + core
        places = [order_in[i, row] for i in range(8)]
        for k in range(8):
            found = jnp.int32(0)
            for i in range(8):
                found = jnp.where(places[i] == k, jnp.int32(i), found)
            place[t * 8 + k] = found

    alpha_rows = 6 + lax.broadcasted_iota(jnp.int32, (8, 128), 0) % 2

    def over(read, store):
        for t in range(2):
            for col in range(2):
                span = pl.ds(col * 128, 128)
                total = read(t, place[t * 8], span)
                for k in range(1, 8):
                    alpha = jnp.take_along_axis(total, alpha_rows, axis=0, mode="promise_in_bounds")
                    total = total + (1.0 - alpha) * read(t, place[t * 8 + k], span)
                store(t, span, total)

    def forward(slot):
        yrel, crel = NEAR[slot]
        return pltpu.make_async_remote_copy(
            src_ref=result.at[slot],
            dst_ref=landed.at[yrel * 2 + core],
            send_sem=send2_sem.at[0],
            recv_sem=recv2_sem.at[slot // 4 + slot // 6],
            device_id=device(x, z, ys[yrel], cores[crel]),
            device_id_type=MESH,
        )

    def pass_on(slot, read):
        def store(t, span, total):
            result[slot, t, :, span] = total

        over(read, store)
        forward(slot).start()

    def land(group):
        part = landed.at[(pl.ds(4, 4), pl.ds(2, 2), pl.ds(0, 1))[group]]
        pltpu.make_async_copy(part, part, recv2_sem.at[group]).wait()

    def put(yrel):
        for t in range(2):
            blocks = [landed[yrel * 2 + c, t, :, pl.ds(col * 128, 128)] for c in range(2) for col in range(2)]
            for ch, rows in enumerate(regroup(blocks, pair)):
                out_ref[ch * 8 + t * 4 + ys[yrel]] = rows

    def store_own(t, span, total):
        landed[core, t, :, span] = total

    for group, slots in enumerate(GROUPS):
        arrive(group)
        for i, slot in enumerate(slots):
            read = lambda t, s, span: received[group][t, s, i, :, span]
            if slot < SLOTS:
                pass_on(slot, read)
            else:
                land(0)
                put(2)
                put(3)
                over(read, store_own)
    land(1)
    put(1)
    land(2)
    put(0)

    part = packed.at[pl.ds(0, PEERS)]
    pltpu.make_async_copy(part, part, send_sem.at[0]).wait()
    part = result.at[pl.ds(0, SLOTS)]
    pltpu.make_async_copy(part, part, send2_sem.at[0]).wait()


def local(voxel_bins, colors, opacity, slab_order):
    f32 = jnp.float32
    out = pl.pallas_call(
        kernel,
        out_shape=pltpu.VMEM((32, 8, 128), f32),
        in_specs=[pl.BlockSpec(memory_space=pl.ANY)] * 4,
        out_specs=pl.BlockSpec(memory_space=pltpu.VMEM),
        scratch_shapes=[
            pltpu.VMEM((2, 8, 16, 8, 256), jnp.int32),
            pltpu.VMEM((3, 256), jnp.bfloat16),
            pltpu.VMEM((256,), jnp.bfloat16),
            pltpu.SMEM((8, 16), jnp.int32),
            pltpu.VMEM((16, 8, 8, 256), f32),
            pltpu.VMEM((8, 2, 8, 256), f32),
            pltpu.VMEM((8, 2, 8, 256), f32),
            pltpu.SMEM((16,), jnp.int32),
            pltpu.SemaphoreType.DMA((3,)),
            pltpu.SemaphoreType.DMA((2,)),
            pltpu.SemaphoreType.DMA((1,)),
            pltpu.SemaphoreType.DMA((len(GROUPS),)),
            pltpu.SemaphoreType.DMA((1,)),
            pltpu.SemaphoreType.DMA((3,)),
            *[pltpu.VMEM((2, 8, len(slots), 8, 256), f32) for slots in GROUPS],
        ],
        compiler_params=pltpu.CompilerParams(collective_id=0, has_side_effects=True),
        name="render_exchange",
    )(voxel_bins.reshape(8, 16, 2, 8, 256), colors, opacity, slab_order.T)
    return jnp.transpose(out.reshape(4, 32, 2, 128), (0, 2, 1, 3)).reshape(4, 2, 4096)


def solution(mesh):
    placed = (P("depth", None, "screen"), P(), P(), P())
    return jax.shard_map(
        local,
        mesh=mesh,
        in_specs=placed,
        out_specs=P(None, ("depth", "screen"), None),
        check_vma=False,
    )
```

```python
import jax
import jax.numpy as jnp
from jax import lax
from jax.experimental import pallas as pl
from jax.experimental.pallas import tpu as pltpu
from jax.sharding import PartitionSpec as P

extinction = 3.0
MESH = pl.DeviceIdType.MESH


def ring(step):
    return min(step, 4 - step)


OFFSETS = sorted(
    [(dx, dz) for dx in range(4) for dz in range(4)],
    key=lambda o: (o == (0, 0), (o[0] * 5 + o[1] * 3) % 11),
)
PEERS = len(OFFSETS) - 1
NEAR = [(2, 0), (2, 1), (3, 0), (3, 1), (1, 0), (1, 1), (0, 1), (0, 0)]
SLOTS = len(NEAR) - 1
GROUPS = [(0, 1, 2, 3), (4, 5), (6,), (7,)]


def coords():
    depth = lax.axis_index("depth")
    screen = lax.axis_index("screen")
    return (
        lax.div(depth, 2),
        lax.rem(depth, 2) * 2 + lax.div(screen, 8),
        lax.rem(lax.div(screen, 2), 4),
        lax.rem(screen, 2),
    )


def device(x, z, y, core):
    return {"depth": x * 2 + lax.div(z, 2), "screen": lax.rem(z, 2) * 8 + y * 2 + core}


def gather_lanes(table, lanes):
    numbers = lax.GatherDimensionNumbers(
        offset_dims=(),
        collapsed_slice_dims=(1,),
        start_index_map=(1,),
        operand_batching_dims=(0,),
        start_indices_batching_dims=(0,),
    )
    return lax.gather(
        table, lanes[..., None], numbers, slice_sizes=(1, 1), mode=lax.GatherScatterMode.PROMISE_IN_BOUNDS
    )


def shade(patches, tables):
    sums = [None] * len(patches)
    for j in range(len(patches[0])):
        for i, bins in enumerate(patches):
            lanes = bins[j] & 127
            low = bins[j] < 128
            values = [
                jnp.where(low, gather_lanes(tables[2 * ch], lanes), gather_lanes(tables[2 * ch + 1], lanes))
                for ch in range(4)
            ]
            if j == 0:
                sums[i] = values
            else:
                clear = 1.0 - sums[i][3]
                sums[i] = [s + clear * v for s, v in zip(sums[i], values)]
    return sums


def regroup(planes, pair):
    low_half = pair < 2
    even = (pair % 2) == 0
    u0 = jnp.where(low_half, planes[0], pltpu.roll(planes[2], 4, 0))
    u1 = jnp.where(low_half, planes[1], pltpu.roll(planes[3], 4, 0))
    v0 = jnp.where(low_half, pltpu.roll(planes[0], 4, 0), planes[2])
    v1 = jnp.where(low_half, pltpu.roll(planes[1], 4, 0), planes[3])
    return [
        jnp.where(even, u0, pltpu.roll(u1, 2, 0)),
        jnp.where(even, pltpu.roll(u0, 6, 0), u1),
        jnp.where(even, v0, pltpu.roll(v1, 2, 0)),
        jnp.where(even, pltpu.roll(v0, 6, 0), v1),
    ]


def kernel(
    vox, colors, opacity, order, out_ref,
    vin, colors_in, opacity_in, order_in, packed, result, landed, place, small_sem, load_sem, send_sem, recv_sem,
    send2_sem, recv2_sem, *received
):
    x, z, y, core = coords()
    half = lax.div(y, 2)
    slab = x * 2 + lax.div(z, 2)
    side = lax.rem(z, 2)
    sibling = y + 1 - 2 * lax.rem(y, 2)
    ys = [y, sibling, lax.rem(y + 2, 4), lax.rem(sibling + 2, 4)]
    cores = [core, 1 - core]

    barrier = pltpu.get_barrier_semaphore()
    for dx, dz in sorted(OFFSETS[:-1], key=lambda o: -(ring(o[0]) + ring(o[1]))):
        pl.semaphore_signal(
            barrier, inc=1, device_id=device(lax.rem(x + dx, 4), lax.rem(z + dz, 4), y, core), device_id_type=MESH
        )
    for yrel, crel in NEAR[:-1]:
        pl.semaphore_signal(barrier, inc=1, device_id=device(x, z, ys[yrel], cores[crel]), device_id_type=MESH)

    def place_of(k):
        dx, dz = OFFSETS[k]
        return lax.rem(x + dx, 4), lax.rem(z + dz, 4)

    def block_of(k):
        to_x, to_z = place_of(k)
        return to_x * 4 + to_z

    def load(k):
        b = block_of(k)
        return pltpu.make_async_copy(vox.at[:, b, 1 - half], vin.at[0, :, b], load_sem.at[min(k // 2, 1)])

    def loaded(count, group):
        part = vin.at[0, :, pl.ds(0, count)]
        return pltpu.make_async_copy(part, part, load_sem.at[group])

    load_own = pltpu.make_async_copy(vox.at[:, :, half], vin.at[1], load_sem.at[2])

    small = [
        pltpu.make_async_copy(colors, colors_in, small_sem.at[0]),
        pltpu.make_async_copy(opacity, opacity_in, small_sem.at[1]),
        pltpu.make_async_copy(order, order_in, small_sem.at[2]),
    ]
    for copy in small[:2]:
        copy.start()
    for k in range(PEERS + 1):
        load(k).start()
    load_own.start()
    small[2].start()

    small[0].wait()
    small[1].wait()
    alpha = 1.0 - jnp.exp(-(extinction / 64) * opacity_in[...].astype(jnp.float32).reshape(1, 256))
    shaded = colors_in[...].astype(jnp.float32) * alpha
    tables = [
        jnp.broadcast_to((shaded[ch : ch + 1] if ch < 3 else alpha)[:, part * 128 : part * 128 + 128], (8, 128))
        for ch in range(4)
        for part in range(2)
    ]
    pair = lax.broadcasted_iota(jnp.int32, (8, 128), 0) // 2

    def render(part, ks):
        blocks = [block_of(k) for k in ks]
        spots = [(b, pl.ds(col * 128, 128)) for b in blocks for col in range(2)]
        for (b, span), planes in zip(
            spots, shade([[vin[part, j, b, :, span] for j in range(8)] for b, span in spots], tables)
        ):
            for q, rows in enumerate(regroup(planes, pair)):
                rel, crel = lax.rem(q // 2 + y, 2), lax.rem(q + core, 2)
                slot = rel * (4 + crel) + (1 - rel) * (7 - crel) if part else rel * 2 + crel
                packed[b, slot, :, span] = rows

    def ends(group, b):
        slots = GROUPS[group]
        return packed.at[b, pl.ds(slots[0], len(slots))], received[group].at[side, slab]

    def message(group, k):
        to_x, to_z = place_of(k)
        source, target = ends(group, to_x * 4 + to_z)
        return pltpu.make_async_remote_copy(
            src_ref=source,
            dst_ref=target,
            send_sem=send_sem.at[0],
            recv_sem=recv_sem.at[group],
            device_id=device(to_x, to_z, y, core),
            device_id_type=MESH,
        )

    def keep(group):
        source, target = ends(group, x * 4 + z)
        return pltpu.make_async_copy(source, target, recv_sem.at[group])

    def send(group, k):
        if k < PEERS:
            message(group, k).start()
        else:
            keep(group).start()

    def arrive(group):
        whole = received[group]
        pltpu.make_async_copy(whole, whole, recv_sem.at[group]).wait()

    for part in range(2):
        if part:
            load_own.wait()
        else:
            loaded(2, 0).wait()
        mine = [g for g, slots in enumerate(GROUPS) if (slots[-1] > 3) == bool(part)]
        for k in range(0, PEERS + 1, 2):
            if part == 0 and k == 2:
                loaded(PEERS - 1, 1).wait()
            render(part, [k, k + 1])
            if part == 0 and k == 0:
                pl.semaphore_wait(barrier, PEERS + SLOTS)
            if part == 0:
                send(0, k)
                send(0, k + 1)
                continue

            @pl.when(core != 1)
            def _():
                send(1, k)
                send(1, k + 1)

        if part:

            @pl.when(core == 1)
            def _():
                for k in range(PEERS + 1):
                    send(1, k)

        for group in mine[1:]:
            for k in range(PEERS + 1):
                send(group, k)

    small[2].wait()
    for t in range(2):
        row = t * 8 + y * 2 + core
        places = [order_in[i, row] for i in range(8)]
        for k in range(8):
            found = jnp.int32(0)
            for i in range(8):
                found = jnp.where(places[i] == k, jnp.int32(i), found)
            place[t * 8 + k] = found

    alpha_rows = 6 + lax.broadcasted_iota(jnp.int32, (8, 128), 0) % 2

    def over(read, store):
        for t in range(2):
            for col in range(2):
                span = pl.ds(col * 128, 128)
                total = read(t, place[t * 8], span)
                for k in range(1, 8):
                    alpha = jnp.take_along_axis(total, alpha_rows, axis=0, mode="promise_in_bounds")
                    total = total + (1.0 - alpha) * read(t, place[t * 8 + k], span)
                store(t, span, total)

    def forward(slot):
        yrel, crel = NEAR[slot]
        return pltpu.make_async_remote_copy(
            src_ref=result.at[slot],
            dst_ref=landed.at[yrel * 2 + core],
            send_sem=send2_sem.at[0],
            recv_sem=recv2_sem.at[slot // 4 + slot // 6],
            device_id=device(x, z, ys[yrel], cores[crel]),
            device_id_type=MESH,
        )

    def pass_on(slot, read):
        def store(t, span, total):
            result[slot, t, :, span] = total

        over(read, store)
        forward(slot).start()

    def land(group):
        part = landed.at[(pl.ds(4, 4), pl.ds(2, 2), pl.ds(0, 1))[group]]
        pltpu.make_async_copy(part, part, recv2_sem.at[group]).wait()

    def put(yrel):
        for t in range(2):
            blocks = [landed[yrel * 2 + c, t, :, pl.ds(col * 128, 128)] for c in range(2) for col in range(2)]
            for ch, rows in enumerate(regroup(blocks, pair)):
                out_ref[ch * 8 + t * 4 + ys[yrel]] = rows

    def store_own(t, span, total):
        landed[core, t, :, span] = total

    for group, slots in enumerate(GROUPS):
        arrive(group)
        for i, slot in enumerate(slots):
            read = lambda t, s, span: received[group][t, s, i, :, span]
            if slot < SLOTS:
                pass_on(slot, read)
            else:
                land(0)
                put(2)
                put(3)
                over(read, store_own)
    land(1)
    put(1)
    land(2)
    put(0)

    part = packed.at[pl.ds(0, PEERS)]
    pltpu.make_async_copy(part, part, send_sem.at[0]).wait()
    part = result.at[pl.ds(0, SLOTS)]
    pltpu.make_async_copy(part, part, send2_sem.at[0]).wait()


def local(voxel_bins, colors, opacity, slab_order):
    f32 = jnp.float32
    out = pl.pallas_call(
        kernel,
        out_shape=pltpu.VMEM((32, 8, 128), f32),
        in_specs=[pl.BlockSpec(memory_space=pl.ANY)] * 4,
        out_specs=pl.BlockSpec(memory_space=pltpu.VMEM),
        scratch_shapes=[
            pltpu.VMEM((2, 8, 16, 8, 256), jnp.int32),
            pltpu.VMEM((3, 256), jnp.bfloat16),
            pltpu.VMEM((256,), jnp.bfloat16),
            pltpu.SMEM((8, 16), jnp.int32),
            pltpu.VMEM((16, 8, 8, 256), f32),
            pltpu.VMEM((8, 2, 8, 256), f32),
            pltpu.VMEM((8, 2, 8, 256), f32),
            pltpu.SMEM((16,), jnp.int32),
            pltpu.SemaphoreType.DMA((3,)),
            pltpu.SemaphoreType.DMA((3,)),
            pltpu.SemaphoreType.DMA((1,)),
            pltpu.SemaphoreType.DMA((len(GROUPS),)),
            pltpu.SemaphoreType.DMA((1,)),
            pltpu.SemaphoreType.DMA((3,)),
            *[pltpu.VMEM((2, 8, len(slots), 8, 256), f32) for slots in GROUPS],
        ],
        compiler_params=pltpu.CompilerParams(collective_id=0, has_side_effects=True),
        name="render_exchange",
    )(voxel_bins.reshape(8, 16, 2, 8, 256), colors, opacity, slab_order.T)
    return jnp.transpose(out.reshape(4, 32, 2, 128), (0, 2, 1, 3)).reshape(4, 2, 4096)


def solution(mesh):
    placed = (P("depth", None, "screen"), P(), P(), P())
    return jax.shard_map(
        local,
        mesh=mesh,
        in_specs=placed,
        out_specs=P(None, ("depth", "screen"), None),
        check_vma=False,
    )
```

```python
import jax
import jax.numpy as jnp
from jax import lax
from jax.experimental import pallas as pl
from jax.experimental.pallas import tpu as pltpu
from jax.sharding import PartitionSpec as P

extinction = 3.0
MESH = pl.DeviceIdType.MESH


def ring(step):
    return min(step, 4 - step)


OFFSETS = sorted(
    [(dx, dz) for dx in range(4) for dz in range(4)],
    key=lambda o: (o == (0, 0), (o[0] * 5 + o[1] * 3) % 11),
)
PEERS = len(OFFSETS) - 1
NEAR = [(2, 0), (2, 1), (3, 0), (3, 1), (1, 0), (1, 1), (0, 1), (0, 0)]
SLOTS = len(NEAR) - 1
GROUPS = [(0, 1, 2, 3), (4, 5), (6,), (7,)]


def coords():
    depth = lax.axis_index("depth")
    screen = lax.axis_index("screen")
    return (
        lax.div(depth, 2),
        lax.rem(depth, 2) * 2 + lax.div(screen, 8),
        lax.rem(lax.div(screen, 2), 4),
        lax.rem(screen, 2),
    )


def device(x, z, y, core):
    return {"depth": x * 2 + lax.div(z, 2), "screen": lax.rem(z, 2) * 8 + y * 2 + core}


def gather_lanes(table, lanes):
    numbers = lax.GatherDimensionNumbers(
        offset_dims=(),
        collapsed_slice_dims=(1,),
        start_index_map=(1,),
        operand_batching_dims=(0,),
        start_indices_batching_dims=(0,),
    )
    return lax.gather(
        table, lanes[..., None], numbers, slice_sizes=(1, 1), mode=lax.GatherScatterMode.PROMISE_IN_BOUNDS
    )


def shade(patches, tables):
    sums = [None] * len(patches)
    for j in range(len(patches[0])):
        for i, bins in enumerate(patches):
            lanes = bins[j] & 127
            low = bins[j] < 128
            values = [
                jnp.where(low, gather_lanes(tables[2 * ch], lanes), gather_lanes(tables[2 * ch + 1], lanes))
                for ch in range(4)
            ]
            if j == 0:
                sums[i] = values
            else:
                clear = 1.0 - sums[i][3]
                sums[i] = [s + clear * v for s, v in zip(sums[i], values)]
    return sums


def regroup(planes, pair):
    low_half = pair < 2
    even = (pair % 2) == 0
    u0 = jnp.where(low_half, planes[0], pltpu.roll(planes[2], 4, 0))
    u1 = jnp.where(low_half, planes[1], pltpu.roll(planes[3], 4, 0))
    v0 = jnp.where(low_half, pltpu.roll(planes[0], 4, 0), planes[2])
    v1 = jnp.where(low_half, pltpu.roll(planes[1], 4, 0), planes[3])
    return [
        jnp.where(even, u0, pltpu.roll(u1, 2, 0)),
        jnp.where(even, pltpu.roll(u0, 6, 0), u1),
        jnp.where(even, v0, pltpu.roll(v1, 2, 0)),
        jnp.where(even, pltpu.roll(v0, 6, 0), v1),
    ]


def kernel(
    vox, colors, opacity, order, out_ref,
    vin, colors_in, opacity_in, order_in, packed, result, landed, place, small_sem, load_sem, send_sem, recv_sem,
    send2_sem, recv2_sem, *received
):
    x, z, y, core = coords()
    half = lax.div(y, 2)
    slab = x * 2 + lax.div(z, 2)
    side = lax.rem(z, 2)
    sibling = y + 1 - 2 * lax.rem(y, 2)
    ys = [y, sibling, lax.rem(y + 2, 4), lax.rem(sibling + 2, 4)]
    cores = [core, 1 - core]

    barrier = pltpu.get_barrier_semaphore()
    for dx, dz in sorted(OFFSETS[:-1], key=lambda o: -(ring(o[0]) + ring(o[1]))):
        pl.semaphore_signal(
            barrier, inc=1, device_id=device(lax.rem(x + dx, 4), lax.rem(z + dz, 4), y, core), device_id_type=MESH
        )
    for yrel, crel in NEAR[:-1]:
        pl.semaphore_signal(barrier, inc=1, device_id=device(x, z, ys[yrel], cores[crel]), device_id_type=MESH)

    def place_of(k):
        dx, dz = OFFSETS[k]
        return lax.rem(x + dx, 4), lax.rem(z + dz, 4)

    def block_of(k):
        to_x, to_z = place_of(k)
        return to_x * 4 + to_z

    def load(k):
        b = block_of(k)
        return pltpu.make_async_copy(vox.at[:, b, 1 - half], vin.at[0, :, b], load_sem.at[min(k // 2, 1)])

    def loaded(count, group):
        part = vin.at[0, :, pl.ds(0, count)]
        return pltpu.make_async_copy(part, part, load_sem.at[group])

    load_own = pltpu.make_async_copy(vox.at[:, :, half], vin.at[1], load_sem.at[2])

    small = [
        pltpu.make_async_copy(colors, colors_in, small_sem.at[0]),
        pltpu.make_async_copy(opacity, opacity_in, small_sem.at[1]),
        pltpu.make_async_copy(order, order_in, small_sem.at[2]),
    ]
    for copy in small[:2]:
        copy.start()
    for k in range(PEERS + 1):
        load(k).start()
    load_own.start()
    small[2].start()

    small[0].wait()
    small[1].wait()
    alpha = 1.0 - jnp.exp(-(extinction / 64) * opacity_in[...].astype(jnp.float32).reshape(1, 256))
    shaded = colors_in[...].astype(jnp.float32) * alpha
    tables = [
        jnp.broadcast_to((shaded[ch : ch + 1] if ch < 3 else alpha)[:, part * 128 : part * 128 + 128], (8, 128))
        for ch in range(4)
        for part in range(2)
    ]
    pair = lax.broadcasted_iota(jnp.int32, (8, 128), 0) // 2

    def render(part, ks):
        blocks = [block_of(k) for k in ks]
        spots = [(b, pl.ds(col * 128, 128)) for b in blocks for col in range(2)]
        for (b, span), planes in zip(
            spots, shade([[vin[part, j, b, :, span] for j in range(8)] for b, span in spots], tables)
        ):
            for q, rows in enumerate(regroup(planes, pair)):
                rel, crel = lax.rem(q // 2 + y, 2), lax.rem(q + core, 2)
                slot = rel * (4 + crel) + (1 - rel) * (7 - crel) if part else rel * 2 + crel
                packed[b, slot, :, span] = rows

    def ends(group, b):
        slots = GROUPS[group]
        return packed.at[b, pl.ds(slots[0], len(slots))], received[group].at[side, slab]

    def message(group, k):
        to_x, to_z = place_of(k)
        source, target = ends(group, to_x * 4 + to_z)
        return pltpu.make_async_remote_copy(
            src_ref=source,
            dst_ref=target,
            send_sem=send_sem.at[0],
            recv_sem=recv_sem.at[group],
            device_id=device(to_x, to_z, y, core),
            device_id_type=MESH,
        )

    def keep(group):
        source, target = ends(group, x * 4 + z)
        return pltpu.make_async_copy(source, target, recv_sem.at[group])

    def send(group, k):
        if k < PEERS:
            message(group, k).start()
        else:
            keep(group).start()

    def arrive(group):
        whole = received[group]
        pltpu.make_async_copy(whole, whole, recv_sem.at[group]).wait()

    for part in range(2):
        if part:
            load_own.wait()
        else:
            loaded(2, 0).wait()
        mine = [g for g, slots in enumerate(GROUPS) if (slots[-1] > 3) == bool(part)]
        for k in range(0, PEERS + 1, 2):
            if part == 0 and k == 2:
                loaded(PEERS - 1, 1).wait()
            render(part, [k, k + 1])
            if part == 0 and k == 0:
                pl.semaphore_wait(barrier, PEERS + SLOTS)
            if part == 0:
                send(0, k)
                send(0, k + 1)
                continue

            @pl.when(core != 1)
            def _():
                send(1, k)
                send(1, k + 1)

        if part:

            @pl.when(core == 1)
            def _():
                for k in range(PEERS + 1):
                    send(1, k)

        for group in mine[1:]:
            for k in range(PEERS + 1):
                send(group, k)

    small[2].wait()
    for t in range(2):
        row = t * 8 + y * 2 + core
        places = [order_in[i, row] for i in range(8)]
        for k in range(8):
            found = jnp.int32(0)
            for i in range(8):
                found = jnp.where(places[i] == k, jnp.int32(i), found)
            place[t * 8 + k] = found

    alpha_rows = 6 + lax.broadcasted_iota(jnp.int32, (8, 128), 0) % 2

    def over(read, store):
        for t in range(2):
            for col in range(2):
                span = pl.ds(col * 128, 128)
                total = read(t, place[t * 8], span)
                for k in range(1, 8):
                    alpha = jnp.take_along_axis(total, alpha_rows, axis=0, mode="promise_in_bounds")
                    total = total + (1.0 - alpha) * read(t, place[t * 8 + k], span)
                store(t, span, total)

    def forward(slot):
        yrel, crel = NEAR[slot]
        return pltpu.make_async_remote_copy(
            src_ref=result.at[slot],
            dst_ref=landed.at[yrel * 2 + core],
            send_sem=send2_sem.at[0],
            recv_sem=recv2_sem.at[slot // 4 + slot // 6],
            device_id=device(x, z, ys[yrel], cores[crel]),
            device_id_type=MESH,
        )

    def pass_on(slot, read):
        def store(t, span, total):
            result[slot, t, :, span] = total

        over(read, store)
        forward(slot).start()

    def land(group):
        part = landed.at[(pl.ds(4, 4), pl.ds(2, 2), pl.ds(0, 1))[group]]
        pltpu.make_async_copy(part, part, recv2_sem.at[group]).wait()

    def put(yrel):
        for t in range(2):
            blocks = [landed[yrel * 2 + c, t, :, pl.ds(col * 128, 128)] for c in range(2) for col in range(2)]
            for ch, rows in enumerate(regroup(blocks, pair)):
                out_ref[ch * 8 + t * 4 + ys[yrel]] = rows

    def store_own(t, span, total):
        landed[core, t, :, span] = total

    for group, slots in enumerate(GROUPS):
        arrive(group)
        for i, slot in reversed(list(enumerate(slots))):
            read = lambda t, s, span: received[group][t, s, i, :, span]
            if slot < SLOTS:
                pass_on(slot, read)
            else:
                land(0)
                put(2)
                put(3)
                over(read, store_own)
    land(1)
    put(1)
    land(2)
    put(0)

    part = packed.at[pl.ds(0, PEERS)]
    pltpu.make_async_copy(part, part, send_sem.at[0]).wait()
    part = result.at[pl.ds(0, SLOTS)]
    pltpu.make_async_copy(part, part, send2_sem.at[0]).wait()


def local(voxel_bins, colors, opacity, slab_order):
    f32 = jnp.float32
    out = pl.pallas_call(
        kernel,
        out_shape=pltpu.VMEM((32, 8, 128), f32),
        in_specs=[pl.BlockSpec(memory_space=pl.ANY)] * 4,
        out_specs=pl.BlockSpec(memory_space=pltpu.VMEM),
        scratch_shapes=[
            pltpu.VMEM((2, 8, 16, 8, 256), jnp.int32),
            pltpu.VMEM((3, 256), jnp.bfloat16),
            pltpu.VMEM((256,), jnp.bfloat16),
            pltpu.SMEM((8, 16), jnp.int32),
            pltpu.VMEM((16, 8, 8, 256), f32),
            pltpu.VMEM((8, 2, 8, 256), f32),
            pltpu.VMEM((8, 2, 8, 256), f32),
            pltpu.SMEM((16,), jnp.int32),
            pltpu.SemaphoreType.DMA((3,)),
            pltpu.SemaphoreType.DMA((3,)),
            pltpu.SemaphoreType.DMA((1,)),
            pltpu.SemaphoreType.DMA((len(GROUPS),)),
            pltpu.SemaphoreType.DMA((1,)),
            pltpu.SemaphoreType.DMA((3,)),
            *[pltpu.VMEM((2, 8, len(slots), 8, 256), f32) for slots in GROUPS],
        ],
        compiler_params=pltpu.CompilerParams(collective_id=0, has_side_effects=True),
        name="render_exchange",
    )(voxel_bins.reshape(8, 16, 2, 8, 256), colors, opacity, slab_order.T)
    return jnp.transpose(out.reshape(4, 32, 2, 128), (0, 2, 1, 3)).reshape(4, 2, 4096)


def solution(mesh):
    placed = (P("depth", None, "screen"), P(), P(), P())
    return jax.shard_map(
        local,
        mesh=mesh,
        in_specs=placed,
        out_specs=P(None, ("depth", "screen"), None),
        check_vma=False,
    )
```

```python
import jax
import jax.numpy as jnp
from jax import lax
from jax.experimental import pallas as pl
from jax.experimental.pallas import tpu as pltpu
from jax.sharding import PartitionSpec as P

extinction = 3.0
MESH = pl.DeviceIdType.MESH


def ring(step):
    return min(step, 4 - step)


OFFSETS = sorted(
    [(dx, dz) for dx in range(4) for dz in range(4)],
    key=lambda o: (o == (0, 0), (o[0] * 5 + o[1] * 3) % 11),
)
PEERS = len(OFFSETS) - 1
NEAR = [(2, 0), (2, 1), (3, 0), (3, 1), (1, 0), (1, 1), (0, 1), (0, 0)]
SLOTS = len(NEAR) - 1
GROUPS = [(0, 1, 2, 3), (4, 5), (6,), (7,)]


def coords():
    depth = lax.axis_index("depth")
    screen = lax.axis_index("screen")
    return (
        lax.div(depth, 2),
        lax.rem(depth, 2) * 2 + lax.div(screen, 8),
        lax.rem(lax.div(screen, 2), 4),
        lax.rem(screen, 2),
    )


def device(x, z, y, core):
    return {"depth": x * 2 + lax.div(z, 2), "screen": lax.rem(z, 2) * 8 + y * 2 + core}


def gather_lanes(table, lanes):
    numbers = lax.GatherDimensionNumbers(
        offset_dims=(),
        collapsed_slice_dims=(1,),
        start_index_map=(1,),
        operand_batching_dims=(0,),
        start_indices_batching_dims=(0,),
    )
    return lax.gather(
        table, lanes[..., None], numbers, slice_sizes=(1, 1), mode=lax.GatherScatterMode.PROMISE_IN_BOUNDS
    )


def shade(patches, tables):
    sums = [None] * len(patches)
    for j in range(len(patches[0])):
        for i, bins in enumerate(patches):
            lanes = bins[j] & 127
            low = bins[j] < 128
            values = [
                jnp.where(low, gather_lanes(tables[2 * ch], lanes), gather_lanes(tables[2 * ch + 1], lanes))
                for ch in range(4)
            ]
            if j == 0:
                sums[i] = values
            else:
                clear = 1.0 - sums[i][3]
                sums[i] = [s + clear * v for s, v in zip(sums[i], values)]
    return sums


def regroup(planes, pair):
    low_half = pair < 2
    even = (pair % 2) == 0
    u0 = jnp.where(low_half, planes[0], pltpu.roll(planes[2], 4, 0))
    u1 = jnp.where(low_half, planes[1], pltpu.roll(planes[3], 4, 0))
    v0 = jnp.where(low_half, pltpu.roll(planes[0], 4, 0), planes[2])
    v1 = jnp.where(low_half, pltpu.roll(planes[1], 4, 0), planes[3])
    return [
        jnp.where(even, u0, pltpu.roll(u1, 2, 0)),
        jnp.where(even, pltpu.roll(u0, 6, 0), u1),
        jnp.where(even, v0, pltpu.roll(v1, 2, 0)),
        jnp.where(even, pltpu.roll(v0, 6, 0), v1),
    ]


def kernel(
    vox, colors, opacity, order, out_ref,
    vin, colors_in, opacity_in, order_in, packed, result, landed, place, small_sem, load_sem, send_sem, recv_sem,
    send2_sem, recv2_sem, *received
):
    x, z, y, core = coords()
    half = lax.div(y, 2)
    slab = x * 2 + lax.div(z, 2)
    side = lax.rem(z, 2)
    sibling = y + 1 - 2 * lax.rem(y, 2)
    ys = [y, sibling, lax.rem(y + 2, 4), lax.rem(sibling + 2, 4)]
    cores = [core, 1 - core]

    barrier = pltpu.get_barrier_semaphore()
    for dx, dz in sorted(OFFSETS[:-1], key=lambda o: -(ring(o[0]) + ring(o[1]))):
        pl.semaphore_signal(
            barrier, inc=1, device_id=device(lax.rem(x + dx, 4), lax.rem(z + dz, 4), y, core), device_id_type=MESH
        )
    for yrel, crel in NEAR[:-1]:
        pl.semaphore_signal(barrier, inc=1, device_id=device(x, z, ys[yrel], cores[crel]), device_id_type=MESH)

    def place_of(k):
        dx, dz = OFFSETS[k]
        return lax.rem(x + dx, 4), lax.rem(z + dz, 4)

    def block_of(k):
        to_x, to_z = place_of(k)
        return to_x * 4 + to_z

    def load(k):
        b = block_of(k)
        return pltpu.make_async_copy(vox.at[:, b, 1 - half], vin.at[0, :, b], load_sem.at[min(k // 2, 1)])

    def loaded(count, group):
        part = vin.at[0, :, pl.ds(0, count)]
        return pltpu.make_async_copy(part, part, load_sem.at[group])

    load_own = pltpu.make_async_copy(vox.at[:, :, half], vin.at[1], load_sem.at[2])

    small = [
        pltpu.make_async_copy(colors, colors_in, small_sem.at[0]),
        pltpu.make_async_copy(opacity, opacity_in, small_sem.at[1]),
        pltpu.make_async_copy(order, order_in, small_sem.at[2]),
    ]
    for copy in small[:2]:
        copy.start()
    for k in range(PEERS + 1):
        load(k).start()
    load_own.start()
    small[2].start()

    small[0].wait()
    small[1].wait()
    alpha = 1.0 - jnp.exp(-(extinction / 64) * opacity_in[...].astype(jnp.float32).reshape(1, 256))
    shaded = colors_in[...].astype(jnp.float32) * alpha
    tables = [
        jnp.broadcast_to((shaded[ch : ch + 1] if ch < 3 else alpha)[:, part * 128 : part * 128 + 128], (8, 128))
        for ch in range(4)
        for part in range(2)
    ]
    pair = lax.broadcasted_iota(jnp.int32, (8, 128), 0) // 2

    def render(part, ks):
        blocks = [block_of(k) for k in ks]
        spots = [(b, pl.ds(col * 128, 128)) for b in blocks for col in range(2)]
        for (b, span), planes in zip(
            spots, shade([[vin[part, j, b, :, span] for j in range(8)] for b, span in spots], tables)
        ):
            for q, rows in enumerate(regroup(planes, pair)):
                rel, crel = lax.rem(q // 2 + y, 2), lax.rem(q + core, 2)
                slot = rel * (4 + crel) + (1 - rel) * (7 - crel) if part else rel * 2 + crel
                packed[b, slot, :, span] = rows

    def ends(group, b):
        slots = GROUPS[group]
        return packed.at[b, pl.ds(slots[0], len(slots))], received[group].at[side, slab]

    def message(group, k):
        to_x, to_z = place_of(k)
        source, target = ends(group, to_x * 4 + to_z)
        return pltpu.make_async_remote_copy(
            src_ref=source,
            dst_ref=target,
            send_sem=send_sem.at[0],
            recv_sem=recv_sem.at[group],
            device_id=device(to_x, to_z, y, core),
            device_id_type=MESH,
        )

    def keep(group):
        source, target = ends(group, x * 4 + z)
        return pltpu.make_async_copy(source, target, recv_sem.at[group])

    def send(group, k):
        if k < PEERS:
            message(group, k).start()
        else:
            keep(group).start()

    def arrive(group):
        whole = received[group]
        pltpu.make_async_copy(whole, whole, recv_sem.at[group]).wait()

    for part in range(2):
        if part:
            load_own.wait()
        else:
            loaded(2, 0).wait()
        mine = [g for g, slots in enumerate(GROUPS) if (slots[-1] > 3) == bool(part)]
        for k in range(0, PEERS + 1, 2):
            if part == 0 and k == 2:
                loaded(PEERS - 1, 1).wait()
            render(part, [k, k + 1])
            if part == 0 and k == 0:
                pl.semaphore_wait(barrier, PEERS + SLOTS)
            if part == 0:
                send(0, k)
                send(0, k + 1)
                continue

            @pl.when(core != 1)
            def _():
                send(1, k)
                send(1, k + 1)

        if part:

            @pl.when(core == 1)
            def _():
                for k in range(PEERS + 1):
                    send(1, k)

        for group in mine[1:]:
            for k in range(PEERS + 1):
                send(group, k)

    small[2].wait()
    for t in range(2):
        row = t * 8 + y * 2 + core
        places = [order_in[i, row] for i in range(8)]
        for k in range(8):
            found = jnp.int32(0)
            for i in range(8):
                found = jnp.where(places[i] == k, jnp.int32(i), found)
            place[t * 8 + k] = found

    alpha_rows = 6 + lax.broadcasted_iota(jnp.int32, (8, 128), 0) % 2

    def over(read, store):
        for t in range(2):
            for col in range(2):
                span = pl.ds(col * 128, 128)
                total = read(t, place[t * 8], span)
                for k in range(1, 8):
                    alpha = jnp.take_along_axis(total, alpha_rows, axis=0, mode="promise_in_bounds")
                    total = total + (1.0 - alpha) * read(t, place[t * 8 + k], span)
                store(t, span, total)

    def forward(slot):
        yrel, crel = NEAR[slot]
        return pltpu.make_async_remote_copy(
            src_ref=result.at[slot],
            dst_ref=landed.at[yrel * 2 + core],
            send_sem=send2_sem.at[0],
            recv_sem=recv2_sem.at[slot // 4 + slot // 6],
            device_id=device(x, z, ys[yrel], cores[crel]),
            device_id_type=MESH,
        )

    def pass_on(slot, read):
        def store(t, span, total):
            result[slot, t, :, span] = total

        over(read, store)
        forward(slot).start()

    def land(group):
        part = landed.at[(pl.ds(4, 4), pl.ds(2, 2), pl.ds(0, 1))[group]]
        pltpu.make_async_copy(part, part, recv2_sem.at[group]).wait()

    def put(yrel):
        for t in range(2):
            blocks = [landed[yrel * 2 + c, t, :, pl.ds(col * 128, 128)] for c in range(2) for col in range(2)]
            for ch, rows in enumerate(regroup(blocks, pair)):
                out_ref[ch * 8 + t * 4 + ys[yrel]] = rows

    def store_own(t, span, total):
        landed[core, t, :, span] = total

    for group, slots in enumerate(GROUPS):
        arrive(group)
        for i, slot in reversed(list(enumerate(slots))):
            read = lambda t, s, span: received[group][t, s, i, :, span]
            if slot < SLOTS:
                pass_on(slot, read)
            else:
                land(0)
                put(2)
                put(3)
                over(read, store_own)
    land(2)
    put(0)
    land(1)
    put(1)

    part = packed.at[pl.ds(0, PEERS)]
    pltpu.make_async_copy(part, part, send_sem.at[0]).wait()
    part = result.at[pl.ds(0, SLOTS)]
    pltpu.make_async_copy(part, part, send2_sem.at[0]).wait()


def local(voxel_bins, colors, opacity, slab_order):
    f32 = jnp.float32
    out = pl.pallas_call(
        kernel,
        out_shape=pltpu.VMEM((32, 8, 128), f32),
        in_specs=[pl.BlockSpec(memory_space=pl.ANY)] * 4,
        out_specs=pl.BlockSpec(memory_space=pltpu.VMEM),
        scratch_shapes=[
            pltpu.VMEM((2, 8, 16, 8, 256), jnp.int32),
            pltpu.VMEM((3, 256), jnp.bfloat16),
            pltpu.VMEM((256,), jnp.bfloat16),
            pltpu.SMEM((8, 16), jnp.int32),
            pltpu.VMEM((16, 8, 8, 256), f32),
            pltpu.VMEM((8, 2, 8, 256), f32),
            pltpu.VMEM((8, 2, 8, 256), f32),
            pltpu.SMEM((16,), jnp.int32),
            pltpu.SemaphoreType.DMA((3,)),
            pltpu.SemaphoreType.DMA((3,)),
            pltpu.SemaphoreType.DMA((1,)),
            pltpu.SemaphoreType.DMA((len(GROUPS),)),
            pltpu.SemaphoreType.DMA((1,)),
            pltpu.SemaphoreType.DMA((3,)),
            *[pltpu.VMEM((2, 8, len(slots), 8, 256), f32) for slots in GROUPS],
        ],
        compiler_params=pltpu.CompilerParams(collective_id=0, has_side_effects=True),
        name="render_exchange",
    )(voxel_bins.reshape(8, 16, 2, 8, 256), colors, opacity, slab_order.T)
    return jnp.transpose(out.reshape(4, 32, 2, 128), (0, 2, 1, 3)).reshape(4, 2, 4096)


def solution(mesh):
    placed = (P("depth", None, "screen"), P(), P(), P())
    return jax.shard_map(
        local,
        mesh=mesh,
        in_specs=placed,
        out_specs=P(None, ("depth", "screen"), None),
        check_vma=False,
    )
```
